32 devices in a mesh: sub: 4 (over y, x), dev: 8 (over z, core).
Axes of the slice: x: 2, y: 2, z: 4, core: 2. Of those that a mesh axis runs over, the one named last changes fastest.
Arguments:
- child_tiles: float32 [8192, 128, 128], P(('sub', 'dev')), parts along dimension 0, may hold values from -6 to 6
- l_slab: float32 [32768, 512], P(('sub', 'dev')), parts along dimension 0, may hold values from -6 to 6
- u_slab: float32 [512, 131072], P(None, ('sub', 'dev')), parts along dimension 1, may hold values from -0.25 to 0.25
- parent_own_entries: float32 [9216, 128, 128], P(('sub', 'dev')), parts along dimension 0, may hold values from -6 to 6
- parent_label: int32 [8, 32], P('sub'), parts along dimension 0, may hold values from 0 to 47, as said below
Outputs:
- parent_front: float32 [9216, 128, 128], P(('sub', 'dev')), parts along dimension 0
The draws below stay inside these ranges and needn't reach their ends.
There are 4 independent parts, one for each index of `sub`. The reference program is written for one: setup_inputs(seed, part) draws one part's arguments, and reference() takes and returns one part's arrays. A program takes and returns all parts, laid end to end along the dimension named above; each array names one. Nothing has to cross between parts.
Inputs may be any that keep to these rules, and one draw needn't show every extreme that they name: `parent_label`: the 32 labels of one child are distinct. For child c and tile row k, the label modulo 8 is sigma((k mod 8 + k // 8 + 4 c) mod 8), with sigma a permutation of 0 to 7 common to both children.
All inputs are finite; a program needn't handle non-finite values.
Results may differ from the reference program's by a relative error of at most 0.000051.
Values sent between devices are 32-bit elements; how exact they have to be, the bound alone decides.
No kernel may reach another device: no remote copies, remote signals or barrier semaphores. Data moves between devices by JAX's collectives and lax.ppermute only.
A program may use at most 128 MiB of HBM per device.

```python
import jax
import jax.numpy as jnp
from jax import lax

TILE_EDGE = 128
MT = 32
PT = 48
PANEL = 512
CGR = 4
PR = 8
CGC = 1
PC = 1
NCD = 4
TPD = 256
PSLOTS = 288
LROWS = 1024
UCOLS = 4096
N_DEV = 8


def draw_parent_label(key, part):
    result = []
    sigma = jax.random.permutation(jax.random.fold_in(key, 7), 8).astype(jnp.int32)
    for child_id in range(2):
        sub_key = jax.random.fold_in(key, 11 + child_id)
        key_score = jax.random.fold_in(sub_key, 2)
        index = jnp.arange(MT, dtype=jnp.int32)
        residue = sigma[(index % 8 + index // 8 + 4 * child_id) % 8]
        scores = jax.random.randint(key_score, (8, PT // 8), 0, 2 ** 20, dtype=jnp.int32)
        scores = scores * (PT // 8) + jnp.arange(PT // 8, dtype=jnp.int32)[None, :]
        chosen = jnp.argsort(scores, axis=1)[:, :MT // 8].astype(jnp.int32)
        quotient = chosen[residue, index // 8]
        result.append(8 * quotient + residue)
    return jnp.stack(result).astype(jnp.int32)


def level_of(stream_key, extent, split, low, largest):
    gain = 1.0
    for axis_at, blocks in split:
        heights = jax.random.uniform(jax.random.fold_in(jax.random.fold_in(stream_key, 6), axis_at), (blocks,), jnp.float32, low / len(split), largest / len(split))
        gain = gain * jnp.repeat(jnp.exp(heights), extent[axis_at] // blocks).reshape((-1,) + (1,) * (len(extent) - 1 - axis_at))
    return gain


def bell_draw(rng, shape, width, most, pieces=(), kind=jnp.bfloat16):
    values = width * jax.random.normal(rng, shape, jnp.float32)
    if pieces:
        values = values * level_of(rng, shape, pieces, -0.22, 0.18)
    return jnp.clip(values, -most, most).astype(kind)


def setup_inputs(seed: int = 0, part: int = 0) -> dict:
    keys = jax.random.split(jax.random.key(seed), 6)
    part_keys = jax.random.split(jax.random.fold_in(keys[5], part), 6)
    return {
        "child_tiles": bell_draw(part_keys[0], (N_DEV * TPD, TILE_EDGE, TILE_EDGE), 1.0, 6.0, ((0, 8),), jnp.float32),
        "l_slab": bell_draw(part_keys[1], (N_DEV * LROWS, PANEL), 1.0, 6.0, ((0, 8),), jnp.float32),
        "u_slab": bell_draw(part_keys[2], (PANEL, N_DEV * UCOLS), PANEL ** -0.5, 0.25, ((1, 8),), jnp.float32),
        "parent_own_entries": bell_draw(part_keys[3], (N_DEV * PSLOTS, TILE_EDGE, TILE_EDGE), 1.0, 6.0, ((0, 8),), jnp.float32),
        "parent_label": draw_parent_label(jax.random.fold_in(jax.random.fold_in(keys[5], part), 71), part),
    }


def reference(child_tiles, l_slab, u_slab, parent_own_entries, parent_label):
    rows_loc = MT // CGR
    cols_loc = MT // CGC
    left_parts = l_slab.reshape(N_DEV, LROWS, PANEL)
    right_parts = u_slab.reshape(PANEL, N_DEV, UCOLS).transpose(1, 0, 2)

    def device_update(pair):
        product = jnp.dot(pair[0], pair[1], precision=lax.Precision.HIGHEST, preferred_element_type=jnp.float32)
        return product.reshape(rows_loc, TILE_EDGE, cols_loc, TILE_EDGE).transpose(0, 2, 1, 3).reshape(TPD, TILE_EDGE, TILE_EDGE)

    products = lax.map(device_update, (left_parts, right_parts)).reshape(N_DEV * TPD, TILE_EDGE, TILE_EDGE)
    updated = child_tiles - products
    glob = jnp.arange(N_DEV * TPD, dtype=jnp.int32)
    device = glob // TPD
    local = glob % TPD
    child_id = device // NCD
    inner = device % NCD
    row_cls = inner // CGC
    col_cls = inner % CGC
    tile_row = row_cls + CGR * (local // cols_loc)
    tile_col = col_cls + CGC * (local % cols_loc)
    label_row = parent_label[child_id, tile_row]
    label_col = parent_label[child_id, tile_col]
    dest_dev = (label_row % PR) * PC + label_col % PC
    dest_slot = (label_row // PR) * (PT // PC) + label_col // PC
    target = (dest_dev * PSLOTS + dest_slot).astype(jnp.int32)
    return parent_own_entries + jax.ops.segment_sum(updated, target, num_segments=N_DEV * PSLOTS)
```

```python
import functools

import jax
import jax.numpy as jnp
from jax import lax
from jax.experimental import pallas as pl
from jax.experimental.pallas import tpu as pltpu
from jax.sharding import PartitionSpec as P


TILE_EDGE = 128
MT = 32
PT = 48
CGR = 4
PR = 8


def row_for(labels, me, ncd, dest):
    child, inner = me // ncd, me % ncd
    row = jnp.int32(0)
    for t in range(MT // CGR):
        row = jnp.where(labels[child, inner + CGR * t] % PR == dest, t, row)
    return row


def parent_row(labels, me, ncd, source):
    child, inner = source // ncd, source % ncd
    row = jnp.int32(0)
    for t in range(MT // CGR):
        label = labels[child, inner + CGR * t]
        row = jnp.where(label % PR == me, label // PR, row)
    return row


def stripe_kernel(labels, me, left, right, child, after, out):
    product = jnp.dot(
        left[...], right[...], precision=lax.Precision.HIGHEST, preferred_element_type=jnp.float32
    )
    for g in range(out.shape[0]):
        out[g] = child[g] - product[:, g * TILE_EDGE : (g + 1) * TILE_EDGE]


def stripe(labels, me, l_slab, u_slab, child_tiles, after, ncd, step, first, count, group):
    panel = l_slab.shape[1]
    groups = MT // group

    def row(lab, who):
        return row_for(lab, who[0], ncd, who[0] ^ step)

    grid_spec = pltpu.PrefetchScalarGridSpec(
        num_scalar_prefetch=2,
        grid=(count // group,),
        in_specs=[
            pl.BlockSpec((TILE_EDGE, panel), lambda j, lab, who: (row(lab, who), 0)),
            pl.BlockSpec((panel, group * TILE_EDGE), lambda j, lab, who: (0, first // group + j)),
            pl.BlockSpec(
                (group, TILE_EDGE, TILE_EDGE),
                lambda j, lab, who: (row(lab, who) * groups + first // group + j, 0, 0),
            ),
            pl.BlockSpec(memory_space=pl.ANY),
        ],
        out_specs=pl.BlockSpec((group, TILE_EDGE, TILE_EDGE), lambda j, lab, who: (j, 0, 0)),
    )
    tile = TILE_EDGE * TILE_EDGE
    return pl.pallas_call(
        stripe_kernel,
        grid_spec=grid_spec,
        out_shape=jax.ShapeDtypeStruct((count, TILE_EDGE, TILE_EDGE), jnp.float32),
        cost_estimate=pl.CostEstimate(
            flops=2 * 6 * count * tile * panel,
            bytes_accessed=4 * (2 * count * tile + TILE_EDGE * panel * (1 + count)),
            transcendentals=0,
        ),
    )(labels, me, l_slab, u_slab, child_tiles, after)


def start_front_kernel(ncd, labels, me, own, tiles, out):
    out[...] = own[...]

    @pl.when(pl.program_id(0) == parent_row(labels, me[0], ncd, me[0]))
    def _():
        def add(j, carry):
            at = labels[me[0] // ncd, j]
            out[at] = out[at] + tiles[j]
            return carry

        lax.fori_loop(0, MT, add, 0)


def start_front(labels, me, own, tiles, ncd):
    block = (PT, TILE_EDGE, TILE_EDGE)
    grid_spec = pltpu.PrefetchScalarGridSpec(
        num_scalar_prefetch=2,
        grid=(own.shape[0] // PT,),
        in_specs=[
            pl.BlockSpec(block, lambda q, lab, who: (q, 0, 0)),
            pl.BlockSpec(tiles.shape, lambda q, lab, who: (0, 0, 0)),
        ],
        out_specs=pl.BlockSpec(block, lambda q, lab, who: (q, 0, 0)),
    )
    return pl.pallas_call(
        functools.partial(start_front_kernel, ncd),
        grid_spec=grid_spec,
        out_shape=jax.ShapeDtypeStruct(own.shape, own.dtype),
        name="start_front",
    )(labels, me, own, tiles)


def each(count, action):
    def one(i, carry):
        action(i)
        return carry

    lax.fori_loop(0, count, one, 0)


def extend_kernel(ncd, step, first, labels, me, tiles, front_in, front, sums, fetched, stored):
    source = me[0] ^ step
    base = parent_row(labels, me[0], ncd, source) * PT
    child = source // ncd
    count = tiles.shape[0]

    def slot(i):
        return front.at[base + labels[child, first + i]]

    def fetch(i):
        return pltpu.make_async_copy(slot(i), sums.at[i], fetched.at[i])

    def store(i):
        return pltpu.make_async_copy(sums.at[i], slot(i), stored.at[i])

    def add(i):
        fetch(i).wait()
        sums[i] = sums[i] + tiles[i]
        store(i).start()

    each(count, lambda i: fetch(i).start())
    each(count, add)
    each(count, lambda i: store(i).wait())


def extend(labels, me, tiles, front, ncd, step, first):
    count = tiles.shape[0]
    grid_spec = pltpu.PrefetchScalarGridSpec(
        num_scalar_prefetch=2,
        grid=(1,),
        in_specs=[
            pl.BlockSpec(tiles.shape, lambda i, lab, who: (0, 0, 0)),
            pl.BlockSpec(memory_space=pl.ANY),
        ],
        out_specs=pl.BlockSpec(memory_space=pl.ANY),
        scratch_shapes=[
            pltpu.VMEM(tiles.shape, jnp.float32),
            pltpu.SemaphoreType.DMA((count,)),
            pltpu.SemaphoreType.DMA((count,)),
        ],
    )
    return pl.pallas_call(
        functools.partial(extend_kernel, ncd, step, first),
        grid_spec=grid_spec,
        out_shape=jax.ShapeDtypeStruct(front.shape, front.dtype),
        input_output_aliases={3: 0},
    )(labels, me, tiles, front)


def take_kernel(ncd, step, first, labels, me, front, out, fetched):
    source = me[0] ^ step
    base = parent_row(labels, me[0], ncd, source) * PT
    child = source // ncd

    def fetch(i):
        slot = base + labels[child, first + i]
        return pltpu.make_async_copy(front.at[slot], out.at[i], fetched.at[i])

    each(out.shape[0], lambda i: fetch(i).start())
    each(out.shape[0], lambda i: fetch(i).wait())


def put_kernel(ncd, step, first, labels, me, tiles, old, front_in, front, sums, stored):
    source = me[0] ^ step
    base = parent_row(labels, me[0], ncd, source) * PT
    child = source // ncd

    def store(i):
        slot = base + labels[child, first + i]
        return pltpu.make_async_copy(sums.at[i], front.at[slot], stored.at[i])

    def add(i):
        sums[i] = old[i] + tiles[i]
        store(i).start()

    each(tiles.shape[0], add)
    each(tiles.shape[0], lambda i: store(i).wait())


def take(labels, me, front, ncd, step, first, count):
    shape = (count, TILE_EDGE, TILE_EDGE)
    grid_spec = pltpu.PrefetchScalarGridSpec(
        num_scalar_prefetch=2,
        grid=(1,),
        in_specs=[pl.BlockSpec(memory_space=pl.ANY)],
        out_specs=pl.BlockSpec(shape, lambda i, lab, who: (0, 0, 0)),
        scratch_shapes=[pltpu.SemaphoreType.DMA((count,))],
    )
    return pl.pallas_call(
        functools.partial(take_kernel, ncd, step, first),
        grid_spec=grid_spec,
        out_shape=jax.ShapeDtypeStruct(shape, jnp.float32),
    )(labels, me, front)


def put(labels, me, tiles, old, front, ncd, step, first):
    block = pl.BlockSpec(tiles.shape, lambda i, lab, who: (0, 0, 0))
    grid_spec = pltpu.PrefetchScalarGridSpec(
        num_scalar_prefetch=2,
        grid=(1,),
        in_specs=[block, block, pl.BlockSpec(memory_space=pl.ANY)],
        out_specs=pl.BlockSpec(memory_space=pl.ANY),
        scratch_shapes=[
            pltpu.VMEM(tiles.shape, jnp.float32),
            pltpu.SemaphoreType.DMA((tiles.shape[0],)),
        ],
    )
    return pl.pallas_call(
        functools.partial(put_kernel, ncd, step, first),
        grid_spec=grid_spec,
        out_shape=jax.ShapeDtypeStruct(front.shape, front.dtype),
        input_output_aliases={4: 0},
    )(labels, me, tiles, old, front)


SENDS = (
    (6, 0, 4, 4),
    (6, 4, 28, 4),
    (4, 0, 32, 8),
    (7, 0, 32, 8),
    (5, 0, 16, 8),
    (5, 16, 12, 4),
    (5, 28, 4, 4),
    (1, 0, 32, 8),
    (2, 0, 32, 8),
    (3, 0, 32, 8),
)
ADDS = ((1, 0), (6, 0), (6, 4), (2, 0), (3, 0), (7, 0), (4, 0), (5, 0), (5, 16))
LAST = (5, 28)


def body_rows(child_tiles, l_slab, u_slab, parent_own_entries, parent_label):
    ndev = lax.axis_size("dev")
    ncd = ndev // 2
    me = lax.axis_index("dev").astype(jnp.int32).reshape(1)
    arrived = {}
    after = parent_label
    for step, first, count, group in SENDS:
        tiles = stripe(
            parent_label, me, l_slab, u_slab, child_tiles, after, ncd, step, first, count, group
        )
        after = tiles
        pairs = [(d, d ^ step) for d in range(ndev)]
        arrived[step, first] = lax.ppermute(tiles, "dev", pairs)
    kept = stripe(parent_label, me, l_slab, u_slab, child_tiles, after, ncd, 0, 0, MT, 8)
    front = start_front(parent_label, me, parent_own_entries, kept, ncd)
    for step, first in ADDS:
        front = extend(parent_label, me, arrived[step, first], front, ncd, step, first)
    step, first = LAST
    tiles = arrived[step, first]
    old = take(parent_label, me, front, ncd, step, first, tiles.shape[0])
    return put(parent_label, me, tiles, old, front, ncd, step, first)


def tile_targets(labels, count, ndev, me_index):
    cgc = ndev // 8
    pcols = ndev // 8
    ncd = ndev // 2
    cols_loc = MT // cgc
    inner = me_index % ncd
    local = jnp.arange(count, dtype=jnp.int32)
    tile_row = inner // cgc + CGR * (local // cols_loc)
    tile_col = inner % cgc + cgc * (local % cols_loc)
    columns = jnp.arange(MT, dtype=jnp.int32)
    label_row = jnp.sum(
        jnp.where(tile_row[:, None] == columns[None, :], labels[None, :], 0), axis=1
    )
    label_col = jnp.sum(
        jnp.where(tile_col[:, None] == columns[None, :], labels[None, :], 0), axis=1
    )
    dest_dev = label_row % PR * pcols + label_col % pcols
    dest_slot = label_row // PR * (PT // pcols) + label_col // pcols
    return (dest_dev, dest_slot)


def update_tiles(child_part, left_rows, u_slab, cols_loc):
    product = jnp.dot(
        left_rows, u_slab, precision=lax.Precision.HIGHEST, preferred_element_type=jnp.float32
    )
    row_tiles = left_rows.shape[0] // TILE_EDGE
    product = (
        product.reshape(row_tiles, TILE_EDGE, cols_loc, TILE_EDGE)
        .transpose(0, 2, 1, 3)
        .reshape(row_tiles * cols_loc, TILE_EDGE, TILE_EDGE)
    )
    return child_part - product


def pack_tiles(updated, dest_dev, dest_slot, ndev, bound):
    count = updated.shape[0]
    order = jnp.arange(count, dtype=jnp.int32)
    earlier = order[None, :] < order[:, None]
    same_dest = dest_dev[:, None] == dest_dev[None, :]
    arrival = jnp.sum(jnp.where(same_dest & earlier, 1, 0), axis=1).astype(jnp.int32)
    position = dest_dev * bound + arrival
    places = jnp.arange(ndev * bound, dtype=jnp.int32)
    hits = places[:, None] == position[None, :]
    select = hits.astype(jnp.float32)
    packed = jnp.dot(
        select,
        updated.reshape(count, -1),
        precision=lax.Precision.HIGHEST,
        preferred_element_type=jnp.float32,
    )
    filled = jnp.sum(jnp.where(hits, 1, 0), axis=1)
    sent_slot = jnp.where(filled > 0, jnp.sum(jnp.where(hits, dest_slot[None, :], 0), axis=1), -1)
    return (packed.reshape(ndev, bound, -1), sent_slot.reshape(ndev, bound))


def assemble_front(incoming_tiles, incoming_slot, slot_count):
    flat = incoming_tiles.reshape(-1, incoming_tiles.shape[-1])
    select = (
        jnp.arange(slot_count, dtype=jnp.int32)[:, None] == incoming_slot.reshape(-1)[None, :]
    ).astype(jnp.float32)
    return jnp.dot(
        select, flat, precision=lax.Precision.HIGHEST, preferred_element_type=jnp.float32
    )


def body_grid(child_tiles, l_slab, u_slab, parent_own_entries, parent_label):
    ndev = lax.axis_size("dev")
    me_index = lax.axis_index("dev")
    cgc = ndev // 8
    pcols = ndev // 8
    bound = max(1, MT // (cgc * pcols))
    cols_loc = MT // cgc
    tiles_dev = child_tiles.shape[0]
    slot_count = parent_own_entries.shape[0]
    child_id = me_index // (ndev // 2)
    labels = lax.dynamic_index_in_dim(parent_label, child_id, 0, keepdims=False)
    updated = update_tiles(child_tiles, l_slab, u_slab, cols_loc)
    dest_dev, dest_slot = tile_targets(labels, tiles_dev, ndev, me_index)
    packed, sent_slot = pack_tiles(updated, dest_dev, dest_slot, ndev, bound)
    incoming_tiles, incoming_slot = (
        lax.all_to_all(packed, "dev", split_axis=0, concat_axis=0, tiled=True),
        lax.all_to_all(sent_slot, "dev", split_axis=0, concat_axis=0, tiled=True),
    )
    summed_entries = assemble_front(incoming_tiles, incoming_slot, slot_count)
    return parent_own_entries + summed_entries.reshape(slot_count, TILE_EDGE, TILE_EDGE)


def solution(mesh):
    in_specs = (
        P(("sub", "dev"), None, None),
        P(("sub", "dev"), None),
        P(None, ("sub", "dev")),
        P(("sub", "dev"), None, None),
        P("sub", None),
    )
    out_specs = P(("sub", "dev"), None, None)
    rows_only = mesh.shape["dev"] == PR
    body = body_rows if rows_only else body_grid
    return jax.shard_map(body, mesh=mesh, in_specs=in_specs, out_specs=out_specs, check_vma=False)
```

```python
import functools

import jax
import jax.numpy as jnp
from jax import lax
from jax.experimental import pallas as pl
from jax.experimental.pallas import tpu as pltpu
from jax.sharding import PartitionSpec as P


TILE_EDGE = 128
MT = 32
PT = 48
CGR = 4
PR = 8
MIB = 1024 * 1024


def row_for(labels, me, ncd, dest):
    child, inner = me // ncd, me % ncd
    row = jnp.int32(0)
    for t in range(MT // CGR):
        row = jnp.where(labels[child, inner + CGR * t] % PR == dest, t, row)
    return row


def parent_row(labels, me, ncd, source):
    child, inner = source // ncd, source % ncd
    row = jnp.int32(0)
    for t in range(MT // CGR):
        label = labels[child, inner + CGR * t]
        row = jnp.where(label % PR == me, label // PR, row)
    return row


def stripe_kernel(labels, me, left, right, child, out):
    product = jnp.dot(
        left[...], right[...], precision=lax.Precision.HIGHEST, preferred_element_type=jnp.float32
    )
    for g in range(out.shape[0]):
        out[g] = child[g] - product[:, g * TILE_EDGE : (g + 1) * TILE_EDGE]


def stripe(labels, me, l_slab, u_slab, child_tiles, ncd, step, first, count, group):
    panel = l_slab.shape[1]
    groups = MT // group

    def row(lab, who):
        return row_for(lab, who[0], ncd, who[0] ^ step)

    grid_spec = pltpu.PrefetchScalarGridSpec(
        num_scalar_prefetch=2,
        grid=(count // group,),
        in_specs=[
            pl.BlockSpec((TILE_EDGE, panel), lambda j, lab, who: (row(lab, who), 0)),
            pl.BlockSpec((panel, group * TILE_EDGE), lambda j, lab, who: (0, first // group + j)),
            pl.BlockSpec(
                (group, TILE_EDGE, TILE_EDGE),
                lambda j, lab, who: (row(lab, who) * groups + first // group + j, 0, 0),
            ),
        ],
        out_specs=pl.BlockSpec((group, TILE_EDGE, TILE_EDGE), lambda j, lab, who: (j, 0, 0)),
    )
    tile = TILE_EDGE * TILE_EDGE
    return pl.pallas_call(
        stripe_kernel,
        grid_spec=grid_spec,
        out_shape=jax.ShapeDtypeStruct((count, TILE_EDGE, TILE_EDGE), jnp.float32),
        cost_estimate=pl.CostEstimate(
            flops=2 * 6 * count * tile * panel,
            bytes_accessed=4 * (2 * count * tile + TILE_EDGE * panel * (1 + count)),
            transcendentals=0,
        ),
    )(labels, me, l_slab, u_slab, child_tiles)


def first_kernel(ncd, step, table, left, right, child, out, labels, rows, columns, sems):
    count = out.shape[0]
    fetch = pltpu.make_async_copy(table, labels, sems.at[0])
    fetch.start()
    fetch_columns = pltpu.make_async_copy(
        right.at[:, pl.ds(0, count * TILE_EDGE)], columns, sems.at[1]
    )
    fetch_columns.start()
    fetch.wait()
    me = lax.axis_index("dev")
    row = row_for(labels, me, ncd, me ^ step)
    fetch_rows = pltpu.make_async_copy(
        left.at[pl.ds(row * TILE_EDGE, TILE_EDGE), :], rows, sems.at[2]
    )
    fetch_rows.start()
    fetch_child = pltpu.make_async_copy(child.at[pl.ds(row * MT, count)], out, sems.at[3])
    fetch_child.start()
    fetch_columns.wait()
    fetch_rows.wait()
    product = jnp.dot(
        rows[...], columns[...], precision=lax.Precision.HIGHEST, preferred_element_type=jnp.float32
    )
    fetch_child.wait()
    for g in range(count):
        out[g] = out[g] - product[:, g * TILE_EDGE : (g + 1) * TILE_EDGE]


def first_tiles(labels, l_slab, u_slab, child_tiles, ncd, step, count):
    shape = (count, TILE_EDGE, TILE_EDGE)
    panel = l_slab.shape[1]
    return pl.pallas_call(
        functools.partial(first_kernel, ncd, step),
        in_specs=[pl.BlockSpec(memory_space=pl.ANY)] * 4,
        out_specs=pl.BlockSpec(memory_space=pltpu.VMEM),
        out_shape=jax.ShapeDtypeStruct(shape, jnp.float32),
        scratch_shapes=[
            pltpu.SMEM(labels.shape, labels.dtype),
            pltpu.VMEM((TILE_EDGE, panel), jnp.float32),
            pltpu.VMEM((panel, count * TILE_EDGE), jnp.float32),
            pltpu.SemaphoreType.DMA((4,)),
        ],
        compiler_params=pltpu.CompilerParams(vmem_limit_bytes=int(62.4 * MIB)),
    )(labels, l_slab, u_slab, child_tiles)


def start_front_kernel(ncd, labels, me, own, tiles, out):
    out[...] = own[...]

    @pl.when(pl.program_id(0) == parent_row(labels, me[0], ncd, me[0]))
    def _():
        def add(j, carry):
            at = labels[me[0] // ncd, j]
            out[at] = out[at] + tiles[j]
            return carry

        lax.fori_loop(0, MT, add, 0)


def start_front(labels, me, own, tiles, ncd):
    block = (PT, TILE_EDGE, TILE_EDGE)
    grid_spec = pltpu.PrefetchScalarGridSpec(
        num_scalar_prefetch=2,
        grid=(own.shape[0] // PT,),
        in_specs=[
            pl.BlockSpec(block, lambda q, lab, who: (q, 0, 0)),
            pl.BlockSpec(tiles.shape, lambda q, lab, who: (0, 0, 0)),
        ],
        out_specs=pl.BlockSpec(block, lambda q, lab, who: (q, 0, 0)),
    )
    return pl.pallas_call(
        functools.partial(start_front_kernel, ncd),
        grid_spec=grid_spec,
        out_shape=jax.ShapeDtypeStruct(own.shape, own.dtype),
        name="start_front",
    )(labels, me, own, tiles)


def each(count, action):
    def one(i, carry):
        action(i)
        return carry

    lax.fori_loop(0, count, one, 0)


def extend_kernel(ncd, step, first, labels, me, tiles, front_in, after, front, sums, fetched, stored):
    source = me[0] ^ step
    base = parent_row(labels, me[0], ncd, source) * PT
    child = source // ncd
    count = tiles.shape[0]

    def slot(i):
        return front.at[base + labels[child, first + i]]

    def fetch(i):
        return pltpu.make_async_copy(slot(i), sums.at[i], fetched.at[i])

    def store(i):
        return pltpu.make_async_copy(sums.at[i], slot(i), stored.at[i])

    def add(i):
        fetch(i).wait()
        sums[i] = sums[i] + tiles[i]
        store(i).start()

    each(count, lambda i: fetch(i).start())
    each(count, add)
    each(count, lambda i: store(i).wait())


def extend(labels, me, tiles, front, after, ncd, step, first):
    count = tiles.shape[0]
    grid_spec = pltpu.PrefetchScalarGridSpec(
        num_scalar_prefetch=2,
        grid=(1,),
        in_specs=[
            pl.BlockSpec(tiles.shape, lambda i, lab, who: (0, 0, 0)),
            pl.BlockSpec(memory_space=pl.ANY),
            pl.BlockSpec(memory_space=pl.ANY),
        ],
        out_specs=pl.BlockSpec(memory_space=pl.ANY),
        scratch_shapes=[
            pltpu.VMEM(tiles.shape, jnp.float32),
            pltpu.SemaphoreType.DMA((count,)),
            pltpu.SemaphoreType.DMA((count,)),
        ],
    )
    return pl.pallas_call(
        functools.partial(extend_kernel, ncd, step, first),
        grid_spec=grid_spec,
        out_shape=jax.ShapeDtypeStruct(front.shape, front.dtype),
        input_output_aliases={3: 0},
        compiler_params=pltpu.CompilerParams(vmem_limit_bytes=8 * MIB),
    )(labels, me, tiles, front, after)


def take_kernel(ncd, step, first, labels, me, front, out, fetched):
    source = me[0] ^ step
    base = parent_row(labels, me[0], ncd, source) * PT
    child = source // ncd

    def fetch(i):
        slot = base + labels[child, first + i]
        return pltpu.make_async_copy(front.at[slot], out.at[i], fetched.at[i])

    each(out.shape[0], lambda i: fetch(i).start())
    each(out.shape[0], lambda i: fetch(i).wait())


def put_kernel(ncd, step, first, labels, me, tiles, old, front_in, front, sums, stored):
    source = me[0] ^ step
    base = parent_row(labels, me[0], ncd, source) * PT
    child = source // ncd

    def store(i):
        slot = base + labels[child, first + i]
        return pltpu.make_async_copy(sums.at[i], front.at[slot], stored.at[i])

    def add(i):
        sums[i] = old[i] + tiles[i]
        store(i).start()

    each(tiles.shape[0], add)
    each(tiles.shape[0], lambda i: store(i).wait())


def take(labels, me, front, ncd, step, first, count):
    shape = (count, TILE_EDGE, TILE_EDGE)
    grid_spec = pltpu.PrefetchScalarGridSpec(
        num_scalar_prefetch=2,
        grid=(1,),
        in_specs=[pl.BlockSpec(memory_space=pl.ANY)],
        out_specs=pl.BlockSpec(shape, lambda i, lab, who: (0, 0, 0)),
        scratch_shapes=[pltpu.SemaphoreType.DMA((count,))],
    )
    return pl.pallas_call(
        functools.partial(take_kernel, ncd, step, first),
        grid_spec=grid_spec,
        out_shape=jax.ShapeDtypeStruct(shape, jnp.float32),
        compiler_params=pltpu.CompilerParams(vmem_limit_bytes=50 * MIB),
    )(labels, me, front)


def put(labels, me, tiles, old, front, ncd, step, first):
    block = pl.BlockSpec(tiles.shape, lambda i, lab, who: (0, 0, 0))
    grid_spec = pltpu.PrefetchScalarGridSpec(
        num_scalar_prefetch=2,
        grid=(1,),
        in_specs=[block, block, pl.BlockSpec(memory_space=pl.ANY)],
        out_specs=pl.BlockSpec(memory_space=pl.ANY),
        scratch_shapes=[
            pltpu.VMEM(tiles.shape, jnp.float32),
            pltpu.SemaphoreType.DMA((tiles.shape[0],)),
        ],
    )
    return pl.pallas_call(
        functools.partial(put_kernel, ncd, step, first),
        grid_spec=grid_spec,
        out_shape=jax.ShapeDtypeStruct(front.shape, front.dtype),
        input_output_aliases={4: 0},
        compiler_params=pltpu.CompilerParams(vmem_limit_bytes=3 * MIB),
    )(labels, me, tiles, old, front)


SENDS = (
    (6, 0, 4, 4),
    (6, 4, 28, 4),
    (4, 0, 32, 8),
    (5, 0, 32, 8),
    (7, 0, 16, 8),
    (7, 16, 12, 4),
    (7, 28, 4, 4),
    (1, 0, 32, 8),
    (2, 0, 32, 8),
    (3, 0, 32, 8),
)
ADDS = ((1, 0), (6, 0), (6, 4), (2, 0), (3, 0), (4, 0), (5, 0), (7, 0), (7, 16))
LAST = (7, 28)


def body_rows(child_tiles, l_slab, u_slab, parent_own_entries, parent_label):
    ndev = lax.axis_size("dev")
    ncd = ndev // 2
    me = lax.axis_index("dev").astype(jnp.int32).reshape(1)
    arrived = {}
    for step, first, count, group in SENDS:
        if not arrived:
            tiles = first_tiles(parent_label, l_slab, u_slab, child_tiles, ncd, step, count)
        else:
            tiles = stripe(
                parent_label,
                me,
                l_slab,
                u_slab,
                child_tiles,
                ncd,
                step,
                first,
                count,
                group,
            )
        pairs = [(d, d ^ step) for d in range(ndev)]
        arrived[step, first] = lax.ppermute(tiles, "dev", pairs)
    kept = stripe(parent_label, me, l_slab, u_slab, child_tiles, ncd, 0, 0, MT, 8)
    front = start_front(parent_label, me, parent_own_entries, kept, ncd)
    for step, first in ADDS[:-1]:
        tiles = arrived[step, first]
        front = extend(parent_label, me, tiles, front, parent_label, ncd, step, first)
    tiles = arrived[LAST]
    old = take(parent_label, me, front, ncd, *LAST, tiles.shape[0])
    step, first = ADDS[-1]
    front = extend(parent_label, me, arrived[step, first], front, old, ncd, step, first)
    return put(parent_label, me, tiles, old, front, ncd, *LAST)


def tile_targets(labels, count, ndev, me_index):
    cgc = ndev // 8
    pcols = ndev // 8
    ncd = ndev // 2
    cols_loc = MT // cgc
    inner = me_index % ncd
    local = jnp.arange(count, dtype=jnp.int32)
    tile_row = inner // cgc + CGR * (local // cols_loc)
    tile_col = inner % cgc + cgc * (local % cols_loc)
    columns = jnp.arange(MT, dtype=jnp.int32)
    label_row = jnp.sum(
        jnp.where(tile_row[:, None] == columns[None, :], labels[None, :], 0), axis=1
    )
    label_col = jnp.sum(
        jnp.where(tile_col[:, None] == columns[None, :], labels[None, :], 0), axis=1
    )
    dest_dev = label_row % PR * pcols + label_col % pcols
    dest_slot = label_row // PR * (PT // pcols) + label_col // pcols
    return (dest_dev, dest_slot)


def update_tiles(child_part, left_rows, u_slab, cols_loc):
    product = jnp.dot(
        left_rows, u_slab, precision=lax.Precision.HIGHEST, preferred_element_type=jnp.float32
    )
    row_tiles = left_rows.shape[0] // TILE_EDGE
    product = (
        product.reshape(row_tiles, TILE_EDGE, cols_loc, TILE_EDGE)
        .transpose(0, 2, 1, 3)
        .reshape(row_tiles * cols_loc, TILE_EDGE, TILE_EDGE)
    )
    return child_part - product


def pack_tiles(updated, dest_dev, dest_slot, ndev, bound):
    count = updated.shape[0]
    order = jnp.arange(count, dtype=jnp.int32)
    earlier = order[None, :] < order[:, None]
    same_dest = dest_dev[:, None] == dest_dev[None, :]
    arrival = jnp.sum(jnp.where(same_dest & earlier, 1, 0), axis=1).astype(jnp.int32)
    position = dest_dev * bound + arrival
    places = jnp.arange(ndev * bound, dtype=jnp.int32)
    hits = places[:, None] == position[None, :]
    select = hits.astype(jnp.float32)
    packed = jnp.dot(
        select,
        updated.reshape(count, -1),
        precision=lax.Precision.HIGHEST,
        preferred_element_type=jnp.float32,
    )
    filled = jnp.sum(jnp.where(hits, 1, 0), axis=1)
    sent_slot = jnp.where(filled > 0, jnp.sum(jnp.where(hits, dest_slot[None, :], 0), axis=1), -1)
    return (packed.reshape(ndev, bound, -1), sent_slot.reshape(ndev, bound))


def assemble_front(incoming_tiles, incoming_slot, slot_count):
    flat = incoming_tiles.reshape(-1, incoming_tiles.shape[-1])
    select = (
        jnp.arange(slot_count, dtype=jnp.int32)[:, None] == incoming_slot.reshape(-1)[None, :]
    ).astype(jnp.float32)
    return jnp.dot(
        select, flat, precision=lax.Precision.HIGHEST, preferred_element_type=jnp.float32
    )


def body_grid(child_tiles, l_slab, u_slab, parent_own_entries, parent_label):
    ndev = lax.axis_size("dev")
    me_index = lax.axis_index("dev")
    cgc = ndev // 8
    pcols = ndev // 8
    bound = max(1, MT // (cgc * pcols))
    cols_loc = MT // cgc
    tiles_dev = child_tiles.shape[0]
    slot_count = parent_own_entries.shape[0]
    child_id = me_index // (ndev // 2)
    labels = lax.dynamic_index_in_dim(parent_label, child_id, 0, keepdims=False)
    updated = update_tiles(child_tiles, l_slab, u_slab, cols_loc)
    dest_dev, dest_slot = tile_targets(labels, tiles_dev, ndev, me_index)
    packed, sent_slot = pack_tiles(updated, dest_dev, dest_slot, ndev, bound)
    incoming_tiles, incoming_slot = (
        lax.all_to_all(packed, "dev", split_axis=0, concat_axis=0, tiled=True),
        lax.all_to_all(sent_slot, "dev", split_axis=0, concat_axis=0, tiled=True),
    )
    summed_entries = assemble_front(incoming_tiles, incoming_slot, slot_count)
    return parent_own_entries + summed_entries.reshape(slot_count, TILE_EDGE, TILE_EDGE)


def solution(mesh):
    in_specs = (
        P(("sub", "dev"), None, None),
        P(("sub", "dev"), None),
        P(None, ("sub", "dev")),
        P(("sub", "dev"), None, None),
        P("sub", None),
    )
    out_specs = P(("sub", "dev"), None, None)
    rows_only = mesh.shape["dev"] == PR
    body = body_rows if rows_only else body_grid
    return jax.shard_map(body, mesh=mesh, in_specs=in_specs, out_specs=out_specs, check_vma=False)
```

```python
import functools

import jax
import jax.numpy as jnp
from jax import lax
from jax.experimental import pallas as pl
from jax.experimental.pallas import tpu as pltpu
from jax.sharding import PartitionSpec as P


TILE_EDGE = 128
MT = 32
PT = 48
CGR = 4
PR = 8
MIB = 1024 * 1024
VMEM_LIMIT = int(62.5 * MIB)


def row_for(labels, me, ncd, dest):
    child, inner = me // ncd, me % ncd
    row = jnp.int32(0)
    for t in range(MT // CGR):
        row = jnp.where(labels[child, inner + CGR * t] % PR == dest, t, row)
    return row


def parent_row(labels, me, ncd, source):
    child, inner = source // ncd, source % ncd
    row = jnp.int32(0)
    for t in range(MT // CGR):
        label = labels[child, inner + CGR * t]
        row = jnp.where(label % PR == me, label // PR, row)
    return row


def stripe_kernel(labels, me, left, right, child, out):
    product = jnp.dot(
        left[...], right[...], precision=lax.Precision.HIGHEST, preferred_element_type=jnp.float32
    )
    for g in range(out.shape[0]):
        out[g] = child[g] - product[:, g * TILE_EDGE : (g + 1) * TILE_EDGE]


def stripe(labels, me, l_slab, u_slab, child_tiles, ncd, step, first, count, group):
    panel = l_slab.shape[1]
    groups = MT // group

    def row(lab, who):
        return row_for(lab, who[0], ncd, who[0] ^ step)

    grid_spec = pltpu.PrefetchScalarGridSpec(
        num_scalar_prefetch=2,
        grid=(count // group,),
        in_specs=[
            pl.BlockSpec((TILE_EDGE, panel), lambda j, lab, who: (row(lab, who), 0)),
            pl.BlockSpec((panel, group * TILE_EDGE), lambda j, lab, who: (0, first // group + j)),
            pl.BlockSpec(
                (group, TILE_EDGE, TILE_EDGE),
                lambda j, lab, who: (row(lab, who) * groups + first // group + j, 0, 0),
            ),
        ],
        out_specs=pl.BlockSpec((group, TILE_EDGE, TILE_EDGE), lambda j, lab, who: (j, 0, 0)),
    )
    tile = TILE_EDGE * TILE_EDGE
    return pl.pallas_call(
        stripe_kernel,
        grid_spec=grid_spec,
        out_shape=jax.ShapeDtypeStruct((count, TILE_EDGE, TILE_EDGE), jnp.float32),
        cost_estimate=pl.CostEstimate(
            flops=2 * 6 * count * tile * panel,
            bytes_accessed=4 * (2 * count * tile + TILE_EDGE * panel * (1 + count)),
            transcendentals=0,
        ),
        compiler_params=pltpu.CompilerParams(vmem_limit_bytes=VMEM_LIMIT),
    )(labels, me, l_slab, u_slab, child_tiles)


def first_kernel(ncd, step, table, left, right, child, out, labels, rows, columns, sems):
    count = out.shape[0]
    fetch = pltpu.make_async_copy(table, labels, sems.at[0])
    fetch.start()
    fetch_columns = pltpu.make_async_copy(
        right.at[:, pl.ds(0, count * TILE_EDGE)], columns, sems.at[1]
    )
    fetch_columns.start()
    fetch.wait()
    me = lax.axis_index("dev")
    row = row_for(labels, me, ncd, me ^ step)
    fetch_rows = pltpu.make_async_copy(
        left.at[pl.ds(row * TILE_EDGE, TILE_EDGE), :], rows, sems.at[2]
    )
    fetch_rows.start()
    fetch_child = pltpu.make_async_copy(child.at[pl.ds(row * MT, count)], out, sems.at[3])
    fetch_child.start()
    fetch_columns.wait()
    fetch_rows.wait()
    product = jnp.dot(
        rows[...], columns[...], precision=lax.Precision.HIGHEST, preferred_element_type=jnp.float32
    )
    fetch_child.wait()
    for g in range(count):
        out[g] = out[g] - product[:, g * TILE_EDGE : (g + 1) * TILE_EDGE]


def first_tiles(labels, l_slab, u_slab, child_tiles, ncd, step, count):
    shape = (count, TILE_EDGE, TILE_EDGE)
    panel = l_slab.shape[1]
    arrays = (labels, l_slab, u_slab, child_tiles)
    return pl.pallas_call(
        functools.partial(first_kernel, ncd, step),
        in_specs=[pl.BlockSpec(memory_space=pl.ANY)] * 4,
        out_specs=pl.BlockSpec(memory_space=pltpu.VMEM),
        out_shape=jax.ShapeDtypeStruct(shape, jnp.float32),
        scratch_shapes=[
            pltpu.SMEM(labels.shape, labels.dtype),
            pltpu.VMEM((TILE_EDGE, panel), jnp.float32),
            pltpu.VMEM((panel, count * TILE_EDGE), jnp.float32),
            pltpu.SemaphoreType.DMA((4,)),
        ],
        compiler_params=pltpu.CompilerParams(vmem_limit_bytes=8 * MIB),
    )(*(pltpu.with_memory_space_constraint(x, pltpu.HBM) for x in arrays))


def start_front_kernel(ncd, labels, me, own, tiles, out):
    out[...] = own[...]

    @pl.when(pl.program_id(0) == parent_row(labels, me[0], ncd, me[0]))
    def _():
        def add(j, carry):
            at = labels[me[0] // ncd, j]
            out[at] = out[at] + tiles[j]
            return carry

        lax.fori_loop(0, MT, add, 0)


def start_front(labels, me, own, tiles, ncd):
    block = (PT, TILE_EDGE, TILE_EDGE)
    grid_spec = pltpu.PrefetchScalarGridSpec(
        num_scalar_prefetch=2,
        grid=(own.shape[0] // PT,),
        in_specs=[
            pl.BlockSpec(block, lambda q, lab, who: (q, 0, 0)),
            pl.BlockSpec(tiles.shape, lambda q, lab, who: (0, 0, 0)),
        ],
        out_specs=pl.BlockSpec(block, lambda q, lab, who: (q, 0, 0)),
    )
    return pl.pallas_call(
        functools.partial(start_front_kernel, ncd),
        grid_spec=grid_spec,
        out_shape=jax.ShapeDtypeStruct(own.shape, own.dtype),
        compiler_params=pltpu.CompilerParams(vmem_limit_bytes=VMEM_LIMIT),
        name="start_front",
    )(labels, me, own, tiles)


def each(count, action):
    def one(i, carry):
        action(i)
        return carry

    lax.fori_loop(0, count, one, 0)


def slots_of(ncd, step, first, labels, me, front):
    source = me ^ step
    base = parent_row(labels, me, ncd, source) * PT
    child = source // ncd
    return lambda i: front.at[base + labels[child, first + i]]


def extend_kernel(ncd, step, first, labels, me, tiles, front_in, after, front, sums, sems):
    slot = slots_of(ncd, step, first, labels, me[0], front)
    count = tiles.shape[0]
    each(count, lambda i: pltpu.make_async_copy(slot(i), sums.at[i], sems.at[0]).start())
    pltpu.make_async_copy(sums, sums, sems.at[0]).wait()

    def add(i):
        sums[i] = sums[i] + tiles[i]
        pltpu.make_async_copy(sums.at[i], slot(i), sems.at[1]).start()

    each(count, add)
    pltpu.make_async_copy(sums, sums, sems.at[1]).wait()


def extend(labels, me, tiles, front, after, ncd, step, first):
    grid_spec = pltpu.PrefetchScalarGridSpec(
        num_scalar_prefetch=2,
        grid=(1,),
        in_specs=[
            pl.BlockSpec(tiles.shape, lambda i, lab, who: (0, 0, 0)),
            pl.BlockSpec(memory_space=pl.ANY),
            pl.BlockSpec(memory_space=pl.ANY),
        ],
        out_specs=pl.BlockSpec(memory_space=pl.ANY),
        scratch_shapes=[
            pltpu.VMEM(tiles.shape, jnp.float32),
            pltpu.SemaphoreType.DMA((2,)),
        ],
    )
    return pl.pallas_call(
        functools.partial(extend_kernel, ncd, step, first),
        grid_spec=grid_spec,
        out_shape=jax.ShapeDtypeStruct(front.shape, front.dtype),
        input_output_aliases={3: 0},
        compiler_params=pltpu.CompilerParams(vmem_limit_bytes=8 * MIB),
    )(labels, me, tiles, front, after)


def take_kernel(ncd, step, first, labels, me, front, out, sem):
    slot = slots_of(ncd, step, first, labels, me[0], front)
    each(out.shape[0], lambda i: pltpu.make_async_copy(slot(i), out.at[i], sem.at[0]).start())
    pltpu.make_async_copy(out, out, sem.at[0]).wait()


def put_kernel(ncd, step, first, labels, me, tiles, old, front_in, front, sums, sem):
    slot = slots_of(ncd, step, first, labels, me[0], front)

    def add(i):
        sums[i] = old[i] + tiles[i]
        pltpu.make_async_copy(sums.at[i], slot(i), sem.at[0]).start()

    each(tiles.shape[0], add)
    pltpu.make_async_copy(sums, sums, sem.at[0]).wait()


def take(labels, me, front, ncd, step, first, count):
    shape = (count, TILE_EDGE, TILE_EDGE)
    grid_spec = pltpu.PrefetchScalarGridSpec(
        num_scalar_prefetch=2,
        grid=(1,),
        in_specs=[pl.BlockSpec(memory_space=pl.ANY)],
        out_specs=pl.BlockSpec(shape, lambda i, lab, who: (0, 0, 0)),
        scratch_shapes=[pltpu.SemaphoreType.DMA((1,))],
    )
    return pl.pallas_call(
        functools.partial(take_kernel, ncd, step, first),
        grid_spec=grid_spec,
        out_shape=jax.ShapeDtypeStruct(shape, jnp.float32),
        compiler_params=pltpu.CompilerParams(vmem_limit_bytes=50 * MIB),
    )(labels, me, front)


def put(labels, me, tiles, old, front, ncd, step, first):
    block = pl.BlockSpec(memory_space=pltpu.VMEM)
    grid_spec = pltpu.PrefetchScalarGridSpec(
        num_scalar_prefetch=2,
        in_specs=[block, block, pl.BlockSpec(memory_space=pl.ANY)],
        out_specs=pl.BlockSpec(memory_space=pl.ANY),
        scratch_shapes=[
            pltpu.VMEM(tiles.shape, jnp.float32),
            pltpu.SemaphoreType.DMA((1,)),
        ],
    )
    return pl.pallas_call(
        functools.partial(put_kernel, ncd, step, first),
        grid_spec=grid_spec,
        out_shape=jax.ShapeDtypeStruct(front.shape, front.dtype),
        input_output_aliases={4: 0},
        compiler_params=pltpu.CompilerParams(vmem_limit_bytes=3 * MIB),
    )(labels, me, tiles, old, front)


SENDS = (
    (6, 0, 4, 4),
    (6, 4, 28, 4),
    (4, 0, 32, 8),
    (5, 0, 32, 8),
    (7, 0, 26, 2),
    (7, 26, 6, 2),
    (1, 0, 32, 8),
    (2, 0, 32, 8),
    (3, 0, 32, 8),
)
ADDS = ((1, 0), (6, 0), (6, 4), (2, 0), (3, 0), (4, 0), (5, 0), (7, 0))
LAST = (7, 26)


def body_rows(child_tiles, l_slab, u_slab, parent_own_entries, parent_label):
    ndev = lax.axis_size("dev")
    ncd = ndev // 2
    me = lax.axis_index("dev").astype(jnp.int32).reshape(1)
    arrived = {}
    for step, first, count, group in SENDS:
        if not arrived:
            tiles = first_tiles(parent_label, l_slab, u_slab, child_tiles, ncd, step, count)
        else:
            tiles = stripe(
                parent_label,
                me,
                l_slab,
                u_slab,
                child_tiles,
                ncd,
                step,
                first,
                count,
                group,
            )
        pairs = [(d, d ^ step) for d in range(ndev)]
        arrived[step, first] = lax.ppermute(tiles, "dev", pairs)
    kept = stripe(parent_label, me, l_slab, u_slab, child_tiles, ncd, 0, 0, MT, 8)
    front = start_front(parent_label, me, parent_own_entries, kept, ncd)
    for step, first in ADDS[:-1]:
        tiles = arrived[step, first]
        front = extend(parent_label, me, tiles, front, parent_label, ncd, step, first)
    tiles = arrived[LAST]
    old = take(parent_label, me, front, ncd, *LAST, tiles.shape[0])
    step, first = ADDS[-1]
    front = extend(parent_label, me, arrived[step, first], front, old, ncd, step, first)
    return put(parent_label, me, tiles, old, front, ncd, *LAST)


def tile_targets(labels, count, ndev, me_index):
    cgc = ndev // 8
    pcols = ndev // 8
    ncd = ndev // 2
    cols_loc = MT // cgc
    inner = me_index % ncd
    local = jnp.arange(count, dtype=jnp.int32)
    tile_row = inner // cgc + CGR * (local // cols_loc)
    tile_col = inner % cgc + cgc * (local % cols_loc)
    columns = jnp.arange(MT, dtype=jnp.int32)
    label_row = jnp.sum(
        jnp.where(tile_row[:, None] == columns[None, :], labels[None, :], 0), axis=1
    )
    label_col = jnp.sum(
        jnp.where(tile_col[:, None] == columns[None, :], labels[None, :], 0), axis=1
    )
    dest_dev = label_row % PR * pcols + label_col % pcols
    dest_slot = label_row // PR * (PT // pcols) + label_col // pcols
    return (dest_dev, dest_slot)


def update_tiles(child_part, left_rows, u_slab, cols_loc):
    product = jnp.dot(
        left_rows, u_slab, precision=lax.Precision.HIGHEST, preferred_element_type=jnp.float32
    )
    row_tiles = left_rows.shape[0] // TILE_EDGE
    product = (
        product.reshape(row_tiles, TILE_EDGE, cols_loc, TILE_EDGE)
        .transpose(0, 2, 1, 3)
        .reshape(row_tiles * cols_loc, TILE_EDGE, TILE_EDGE)
    )
    return child_part - product


def pack_tiles(updated, dest_dev, dest_slot, ndev, bound):
    count = updated.shape[0]
    order = jnp.arange(count, dtype=jnp.int32)
    earlier = order[None, :] < order[:, None]
    same_dest = dest_dev[:, None] == dest_dev[None, :]
    arrival = jnp.sum(jnp.where(same_dest & earlier, 1, 0), axis=1).astype(jnp.int32)
    position = dest_dev * bound + arrival
    places = jnp.arange(ndev * bound, dtype=jnp.int32)
    hits = places[:, None] == position[None, :]
    select = hits.astype(jnp.float32)
    packed = jnp.dot(
        select,
        updated.reshape(count, -1),
        precision=lax.Precision.HIGHEST,
        preferred_element_type=jnp.float32,
    )
    filled = jnp.sum(jnp.where(hits, 1, 0), axis=1)
    sent_slot = jnp.where(filled > 0, jnp.sum(jnp.where(hits, dest_slot[None, :], 0), axis=1), -1)
    return (packed.reshape(ndev, bound, -1), sent_slot.reshape(ndev, bound))


def assemble_front(incoming_tiles, incoming_slot, slot_count):
    flat = incoming_tiles.reshape(-1, incoming_tiles.shape[-1])
    select = (
        jnp.arange(slot_count, dtype=jnp.int32)[:, None] == incoming_slot.reshape(-1)[None, :]
    ).astype(jnp.float32)
    return jnp.dot(
        select, flat, precision=lax.Precision.HIGHEST, preferred_element_type=jnp.float32
    )


def body_grid(child_tiles, l_slab, u_slab, parent_own_entries, parent_label):
    ndev = lax.axis_size("dev")
    me_index = lax.axis_index("dev")
    cgc = ndev // 8
    pcols = ndev // 8
    bound = max(1, MT // (cgc * pcols))
    cols_loc = MT // cgc
    tiles_dev = child_tiles.shape[0]
    slot_count = parent_own_entries.shape[0]
    child_id = me_index // (ndev // 2)
    labels = lax.dynamic_index_in_dim(parent_label, child_id, 0, keepdims=False)
    updated = update_tiles(child_tiles, l_slab, u_slab, cols_loc)
    dest_dev, dest_slot = tile_targets(labels, tiles_dev, ndev, me_index)
    packed, sent_slot = pack_tiles(updated, dest_dev, dest_slot, ndev, bound)
    incoming_tiles, incoming_slot = (
        lax.all_to_all(packed, "dev", split_axis=0, concat_axis=0, tiled=True),
        lax.all_to_all(sent_slot, "dev", split_axis=0, concat_axis=0, tiled=True),
    )
    summed_entries = assemble_front(incoming_tiles, incoming_slot, slot_count)
    return parent_own_entries + summed_entries.reshape(slot_count, TILE_EDGE, TILE_EDGE)


def solution(mesh):
    in_specs = (
        P(("sub", "dev"), None, None),
        P(("sub", "dev"), None),
        P(None, ("sub", "dev")),
        P(("sub", "dev"), None, None),
        P("sub", None),
    )
    out_specs = P(("sub", "dev"), None, None)
    rows_only = mesh.shape["dev"] == PR
    body = body_rows if rows_only else body_grid
    return jax.shard_map(body, mesh=mesh, in_specs=in_specs, out_specs=out_specs, check_vma=False)
```

```python
import functools

import jax
import jax.numpy as jnp
from jax import lax
from jax.experimental import pallas as pl
from jax.experimental.pallas import tpu as pltpu
from jax.sharding import PartitionSpec as P


TILE_EDGE = 128
MT = 32
PT = 48
CGR = 4
PR = 8
MIB = 1024 * 1024
VMEM_LIMIT = 24 * MIB


def in_hbm(x):
    return pltpu.with_memory_space_constraint(x, pltpu.HBM)


def row_for(labels, me, ncd, dest):
    child, inner = me // ncd, me % ncd
    row = jnp.int32(0)
    for t in range(MT // CGR):
        row = jnp.where(labels[child, inner + CGR * t] % PR == dest, t, row)
    return row


def parent_row(labels, me, ncd, source):
    child, inner = source // ncd, source % ncd
    row = jnp.int32(0)
    for t in range(MT // CGR):
        label = labels[child, inner + CGR * t]
        row = jnp.where(label % PR == me, label // PR, row)
    return row


def stripe_kernel(labels, me, left, right, child, out):
    product = jnp.dot(
        left[...], right[...], precision=lax.Precision.HIGHEST, preferred_element_type=jnp.float32
    )
    for g in range(out.shape[0]):
        out[g] = child[g] - product[:, g * TILE_EDGE : (g + 1) * TILE_EDGE]


def stripe(labels, me, l_slab, u_slab, child_tiles, ncd, step, first, count, group):
    panel = l_slab.shape[1]
    groups = MT // group

    def row(lab, who):
        return row_for(lab, who[0], ncd, who[0] ^ step)

    grid_spec = pltpu.PrefetchScalarGridSpec(
        num_scalar_prefetch=2,
        grid=(count // group,),
        in_specs=[
            pl.BlockSpec((TILE_EDGE, panel), lambda j, lab, who: (row(lab, who), 0)),
            pl.BlockSpec((panel, group * TILE_EDGE), lambda j, lab, who: (0, first // group + j)),
            pl.BlockSpec(
                (group, TILE_EDGE, TILE_EDGE),
                lambda j, lab, who: (row(lab, who) * groups + first // group + j, 0, 0),
            ),
        ],
        out_specs=pl.BlockSpec((group, TILE_EDGE, TILE_EDGE), lambda j, lab, who: (j, 0, 0)),
    )
    tile = TILE_EDGE * TILE_EDGE
    return pl.pallas_call(
        stripe_kernel,
        grid_spec=grid_spec,
        out_shape=jax.ShapeDtypeStruct((count, TILE_EDGE, TILE_EDGE), jnp.float32),
        cost_estimate=pl.CostEstimate(
            flops=2 * 6 * count * tile * panel,
            bytes_accessed=4 * (2 * count * tile + TILE_EDGE * panel * (1 + count)),
            transcendentals=0,
        ),
        compiler_params=pltpu.CompilerParams(vmem_limit_bytes=VMEM_LIMIT),
    )(in_hbm(labels), me, *(in_hbm(x) for x in (l_slab, u_slab, child_tiles)))


def first_kernel(ncd, step, table, left, right, child, out, labels, rows, columns, sems):
    count = out.shape[0]
    fetch = pltpu.make_async_copy(table, labels, sems.at[0])
    fetch.start()
    fetch_columns = pltpu.make_async_copy(
        right.at[:, pl.ds(0, count * TILE_EDGE)], columns, sems.at[1]
    )
    fetch_columns.start()
    fetch.wait()
    me = lax.axis_index("dev")
    row = row_for(labels, me, ncd, me ^ step)
    fetch_rows = pltpu.make_async_copy(
        left.at[pl.ds(row * TILE_EDGE, TILE_EDGE), :], rows, sems.at[2]
    )
    fetch_rows.start()
    fetch_child = pltpu.make_async_copy(child.at[pl.ds(row * MT, count)], out, sems.at[3])
    fetch_child.start()
    fetch_columns.wait()
    fetch_rows.wait()
    product = jnp.dot(
        rows[...], columns[...], precision=lax.Precision.HIGHEST, preferred_element_type=jnp.float32
    )
    fetch_child.wait()
    for g in range(count):
        out[g] = out[g] - product[:, g * TILE_EDGE : (g + 1) * TILE_EDGE]


def first_tiles(labels, l_slab, u_slab, child_tiles, ncd, step, count):
    shape = (count, TILE_EDGE, TILE_EDGE)
    panel = l_slab.shape[1]
    arrays = (labels, l_slab, u_slab, child_tiles)
    return pl.pallas_call(
        functools.partial(first_kernel, ncd, step),
        in_specs=[pl.BlockSpec(memory_space=pl.ANY)] * 4,
        out_specs=pl.BlockSpec(memory_space=pltpu.VMEM),
        out_shape=jax.ShapeDtypeStruct(shape, jnp.float32),
        scratch_shapes=[
            pltpu.SMEM(labels.shape, labels.dtype),
            pltpu.VMEM((TILE_EDGE, panel), jnp.float32),
            pltpu.VMEM((panel, count * TILE_EDGE), jnp.float32),
            pltpu.SemaphoreType.DMA((4,)),
        ],
        compiler_params=pltpu.CompilerParams(vmem_limit_bytes=8 * MIB),
    )(*(in_hbm(x) for x in arrays))


def start_front_kernel(ncd, labels, me, own, tiles, out):
    out[...] = own[...]

    @pl.when(pl.program_id(0) == parent_row(labels, me[0], ncd, me[0]))
    def _():
        def add(j, carry):
            at = labels[me[0] // ncd, j]
            out[at] = out[at] + tiles[j]
            return carry

        lax.fori_loop(0, MT, add, 0)


def start_front(labels, me, own, tiles, ncd):
    block = (PT, TILE_EDGE, TILE_EDGE)
    grid_spec = pltpu.PrefetchScalarGridSpec(
        num_scalar_prefetch=2,
        grid=(own.shape[0] // PT,),
        in_specs=[
            pl.BlockSpec(block, lambda q, lab, who: (q, 0, 0)),
            pl.BlockSpec(tiles.shape, lambda q, lab, who: (0, 0, 0)),
        ],
        out_specs=pl.BlockSpec(block, lambda q, lab, who: (q, 0, 0)),
    )
    return pl.pallas_call(
        functools.partial(start_front_kernel, ncd),
        grid_spec=grid_spec,
        out_shape=jax.ShapeDtypeStruct(own.shape, own.dtype),
        compiler_params=pltpu.CompilerParams(vmem_limit_bytes=VMEM_LIMIT),
        name="start_front",
    )(labels, me, in_hbm(own), tiles)


def each(count, action):
    def one(i, carry):
        action(i)
        return carry

    lax.fori_loop(0, count, one, 0)


def slots_of(ncd, step, first, labels, me, front):
    source = me ^ step
    base = parent_row(labels, me, ncd, source) * PT
    child = source // ncd
    return lambda i: front.at[base + labels[child, first + i]]


def extend_kernel(ncd, step, first, labels, me, tiles, front_in, after, front, sums, sems):
    slot = slots_of(ncd, step, first, labels, me[0], front)
    count = tiles.shape[0]
    each(count, lambda i: pltpu.make_async_copy(slot(i), sums.at[i], sems.at[0]).start())
    pltpu.make_async_copy(sums, sums, sems.at[0]).wait()

    def add(i):
        sums[i] = sums[i] + tiles[i]
        pltpu.make_async_copy(sums.at[i], slot(i), sems.at[1]).start()

    each(count, add)
    pltpu.make_async_copy(sums, sums, sems.at[1]).wait()


def extend(labels, me, tiles, front, after, ncd, step, first):
    grid_spec = pltpu.PrefetchScalarGridSpec(
        num_scalar_prefetch=2,
        grid=(1,),
        in_specs=[
            pl.BlockSpec(tiles.shape, lambda i, lab, who: (0, 0, 0)),
            pl.BlockSpec(memory_space=pl.ANY),
            pl.BlockSpec(memory_space=pl.ANY),
        ],
        out_specs=pl.BlockSpec(memory_space=pl.ANY),
        scratch_shapes=[
            pltpu.VMEM(tiles.shape, jnp.float32),
            pltpu.SemaphoreType.DMA((2,)),
        ],
    )
    return pl.pallas_call(
        functools.partial(extend_kernel, ncd, step, first),
        grid_spec=grid_spec,
        out_shape=jax.ShapeDtypeStruct(front.shape, front.dtype),
        input_output_aliases={3: 0},
        compiler_params=pltpu.CompilerParams(vmem_limit_bytes=8 * MIB),
    )(labels, me, tiles, front, after)


def take_kernel(ncd, step, first, labels, me, front, out, sem):
    slot = slots_of(ncd, step, first, labels, me[0], front)
    each(out.shape[0], lambda i: pltpu.make_async_copy(slot(i), out.at[i], sem.at[0]).start())
    pltpu.make_async_copy(out, out, sem.at[0]).wait()


def put_kernel(ncd, step, first, labels, me, tiles, old, front_in, front, sums, sem):
    slot = slots_of(ncd, step, first, labels, me[0], front)

    def add(i):
        sums[i] = old[i] + tiles[i]
        pltpu.make_async_copy(sums.at[i], slot(i), sem.at[0]).start()

    each(tiles.shape[0], add)
    pltpu.make_async_copy(sums, sums, sem.at[0]).wait()


def take(labels, me, front, ncd, step, first, count):
    shape = (count, TILE_EDGE, TILE_EDGE)
    grid_spec = pltpu.PrefetchScalarGridSpec(
        num_scalar_prefetch=2,
        grid=(1,),
        in_specs=[pl.BlockSpec(memory_space=pl.ANY)],
        out_specs=pl.BlockSpec(shape, lambda i, lab, who: (0, 0, 0)),
        scratch_shapes=[pltpu.SemaphoreType.DMA((1,))],
    )
    return pl.pallas_call(
        functools.partial(take_kernel, ncd, step, first),
        grid_spec=grid_spec,
        out_shape=jax.ShapeDtypeStruct(shape, jnp.float32),
        compiler_params=pltpu.CompilerParams(vmem_limit_bytes=50 * MIB),
    )(labels, me, in_hbm(front))


def put(labels, me, tiles, old, front, ncd, step, first):
    block = pl.BlockSpec(memory_space=pltpu.VMEM)
    grid_spec = pltpu.PrefetchScalarGridSpec(
        num_scalar_prefetch=2,
        in_specs=[block, block, pl.BlockSpec(memory_space=pl.ANY)],
        out_specs=pl.BlockSpec(memory_space=pl.ANY),
        scratch_shapes=[
            pltpu.VMEM(tiles.shape, jnp.float32),
            pltpu.SemaphoreType.DMA((1,)),
        ],
    )
    return pl.pallas_call(
        functools.partial(put_kernel, ncd, step, first),
        grid_spec=grid_spec,
        out_shape=jax.ShapeDtypeStruct(front.shape, front.dtype),
        input_output_aliases={4: 0},
        compiler_params=pltpu.CompilerParams(vmem_limit_bytes=3 * MIB),
    )(labels, me, tiles, old, front)


SENDS = (
    (6, 0, 4, 4),
    (6, 4, 28, 4),
    (4, 0, 32, 8),
    (5, 0, 32, 8),
    (7, 0, 28, 4),
    (7, 28, 4, 4),
    (1, 0, 32, 8),
    (2, 0, 32, 8),
    (3, 0, 32, 8),
)
ADDS = ((1, 0), (6, 0), (6, 4), (2, 0), (3, 0), (4, 0), (5, 0), (7, 0))
LAST = (7, 28)


def body_rows(child_tiles, l_slab, u_slab, parent_own_entries, parent_label):
    ndev = lax.axis_size("dev")
    ncd = ndev // 2
    me = lax.axis_index("dev").astype(jnp.int32).reshape(1)
    arrived = {}
    for step, first, count, group in SENDS:
        if not arrived:
            tiles = first_tiles(parent_label, l_slab, u_slab, child_tiles, ncd, step, count)
        else:
            tiles = stripe(
                parent_label,
                me,
                l_slab,
                u_slab,
                child_tiles,
                ncd,
                step,
                first,
                count,
                group,
            )
        pairs = [(d, d ^ step) for d in range(ndev)]
        arrived[step, first] = lax.ppermute(tiles, "dev", pairs)
    kept = stripe(parent_label, me, l_slab, u_slab, child_tiles, ncd, 0, 0, MT, 8)
    front = start_front(parent_label, me, parent_own_entries, kept, ncd)
    for step, first in ADDS[:-1]:
        tiles = arrived[step, first]
        front = extend(parent_label, me, tiles, front, parent_label, ncd, step, first)
    tiles = arrived[LAST]
    old = take(parent_label, me, front, ncd, *LAST, tiles.shape[0])
    step, first = ADDS[-1]
    front = extend(parent_label, me, arrived[step, first], front, old, ncd, step, first)
    return put(parent_label, me, tiles, old, front, ncd, *LAST)


def tile_targets(labels, count, ndev, me_index):
    cgc = ndev // 8
    pcols = ndev // 8
    ncd = ndev // 2
    cols_loc = MT // cgc
    inner = me_index % ncd
    local = jnp.arange(count, dtype=jnp.int32)
    tile_row = inner // cgc + CGR * (local // cols_loc)
    tile_col = inner % cgc + cgc * (local % cols_loc)
    columns = jnp.arange(MT, dtype=jnp.int32)
    label_row = jnp.sum(
        jnp.where(tile_row[:, None] == columns[None, :], labels[None, :], 0), axis=1
    )
    label_col = jnp.sum(
        jnp.where(tile_col[:, None] == columns[None, :], labels[None, :], 0), axis=1
    )
    dest_dev = label_row % PR * pcols + label_col % pcols
    dest_slot = label_row // PR * (PT // pcols) + label_col // pcols
    return (dest_dev, dest_slot)


def update_tiles(child_part, left_rows, u_slab, cols_loc):
    product = jnp.dot(
        left_rows, u_slab, precision=lax.Precision.HIGHEST, preferred_element_type=jnp.float32
    )
    row_tiles = left_rows.shape[0] // TILE_EDGE
    product = (
        product.reshape(row_tiles, TILE_EDGE, cols_loc, TILE_EDGE)
        .transpose(0, 2, 1, 3)
        .reshape(row_tiles * cols_loc, TILE_EDGE, TILE_EDGE)
    )
    return child_part - product


def pack_tiles(updated, dest_dev, dest_slot, ndev, bound):
    count = updated.shape[0]
    order = jnp.arange(count, dtype=jnp.int32)
    earlier = order[None, :] < order[:, None]
    same_dest = dest_dev[:, None] == dest_dev[None, :]
    arrival = jnp.sum(jnp.where(same_dest & earlier, 1, 0), axis=1).astype(jnp.int32)
    position = dest_dev * bound + arrival
    places = jnp.arange(ndev * bound, dtype=jnp.int32)
    hits = places[:, None] == position[None, :]
    select = hits.astype(jnp.float32)
    packed = jnp.dot(
        select,
        updated.reshape(count, -1),
        precision=lax.Precision.HIGHEST,
        preferred_element_type=jnp.float32,
    )
    filled = jnp.sum(jnp.where(hits, 1, 0), axis=1)
    sent_slot = jnp.where(filled > 0, jnp.sum(jnp.where(hits, dest_slot[None, :], 0), axis=1), -1)
    return (packed.reshape(ndev, bound, -1), sent_slot.reshape(ndev, bound))


def assemble_front(incoming_tiles, incoming_slot, slot_count):
    flat = incoming_tiles.reshape(-1, incoming_tiles.shape[-1])
    select = (
        jnp.arange(slot_count, dtype=jnp.int32)[:, None] == incoming_slot.reshape(-1)[None, :]
    ).astype(jnp.float32)
    return jnp.dot(
        select, flat, precision=lax.Precision.HIGHEST, preferred_element_type=jnp.float32
    )


def body_grid(child_tiles, l_slab, u_slab, parent_own_entries, parent_label):
    ndev = lax.axis_size("dev")
    me_index = lax.axis_index("dev")
    cgc = ndev // 8
    pcols = ndev // 8
    bound = max(1, MT // (cgc * pcols))
    cols_loc = MT // cgc
    tiles_dev = child_tiles.shape[0]
    slot_count = parent_own_entries.shape[0]
    child_id = me_index // (ndev // 2)
    labels = lax.dynamic_index_in_dim(parent_label, child_id, 0, keepdims=False)
    updated = update_tiles(child_tiles, l_slab, u_slab, cols_loc)
    dest_dev, dest_slot = tile_targets(labels, tiles_dev, ndev, me_index)
    packed, sent_slot = pack_tiles(updated, dest_dev, dest_slot, ndev, bound)
    incoming_tiles, incoming_slot = (
        lax.all_to_all(packed, "dev", split_axis=0, concat_axis=0, tiled=True),
        lax.all_to_all(sent_slot, "dev", split_axis=0, concat_axis=0, tiled=True),
    )
    summed_entries = assemble_front(incoming_tiles, incoming_slot, slot_count)
    return parent_own_entries + summed_entries.reshape(slot_count, TILE_EDGE, TILE_EDGE)


def solution(mesh):
    in_specs = (
        P(("sub", "dev"), None, None),
        P(("sub", "dev"), None),
        P(None, ("sub", "dev")),
        P(("sub", "dev"), None, None),
        P("sub", None),
    )
    out_specs = P(("sub", "dev"), None, None)
    rows_only = mesh.shape["dev"] == PR
    body = body_rows if rows_only else body_grid
    return jax.shard_map(body, mesh=mesh, in_specs=in_specs, out_specs=out_specs, check_vma=False)
```

```python
import functools

import jax
import jax.numpy as jnp
from jax import lax
from jax.experimental import pallas as pl
from jax.experimental.pallas import tpu as pltpu
from jax.sharding import PartitionSpec as P


TILE_EDGE = 128
MT = 32
PT = 48
CGR = 4
PR = 8
MIB = 1024 * 1024
VMEM_LIMIT = 24 * MIB


def in_hbm(x):
    return pltpu.with_memory_space_constraint(x, pltpu.HBM)


def row_for(labels, me, ncd, dest):
    child, inner = me // ncd, me % ncd
    row = jnp.int32(0)
    for t in range(MT // CGR):
        row = jnp.where(labels[child, inner + CGR * t] % PR == dest, t, row)
    return row


def parent_row(labels, me, ncd, source):
    child, inner = source // ncd, source % ncd
    row = jnp.int32(0)
    for t in range(MT // CGR):
        label = labels[child, inner + CGR * t]
        row = jnp.where(label % PR == me, label // PR, row)
    return row


def stripe_kernel(labels, me, left, right, child, out):
    product = jnp.dot(
        left[...], right[...], precision=lax.Precision.HIGHEST, preferred_element_type=jnp.float32
    )
    for g in range(out.shape[0]):
        out[g] = child[g] - product[:, g * TILE_EDGE : (g + 1) * TILE_EDGE]


def stripe(labels, me, l_slab, u_slab, child_tiles, ncd, step, first, count, group):
    panel = l_slab.shape[1]
    groups = MT // group

    def row(lab, who):
        return row_for(lab, who[0], ncd, who[0] ^ step)

    grid_spec = pltpu.PrefetchScalarGridSpec(
        num_scalar_prefetch=2,
        grid=(count // group,),
        in_specs=[
            pl.BlockSpec((TILE_EDGE, panel), lambda j, lab, who: (row(lab, who), 0)),
            pl.BlockSpec((panel, group * TILE_EDGE), lambda j, lab, who: (0, first // group + j)),
            pl.BlockSpec(
                (group, TILE_EDGE, TILE_EDGE),
                lambda j, lab, who: (row(lab, who) * groups + first // group + j, 0, 0),
            ),
        ],
        out_specs=pl.BlockSpec((group, TILE_EDGE, TILE_EDGE), lambda j, lab, who: (j, 0, 0)),
    )
    tile = TILE_EDGE * TILE_EDGE
    return pl.pallas_call(
        stripe_kernel,
        grid_spec=grid_spec,
        out_shape=jax.ShapeDtypeStruct((count, TILE_EDGE, TILE_EDGE), jnp.float32),
        cost_estimate=pl.CostEstimate(
            flops=2 * 6 * count * tile * panel,
            bytes_accessed=4 * (2 * count * tile + TILE_EDGE * panel * (1 + count)),
            transcendentals=0,
        ),
        compiler_params=pltpu.CompilerParams(vmem_limit_bytes=VMEM_LIMIT),
    )(in_hbm(labels), me, *(in_hbm(x) for x in (l_slab, u_slab, child_tiles)))


def first_kernel(ncd, step, table, left, right, child, out, labels, rows, columns, sems):
    count = out.shape[0]
    fetch = pltpu.make_async_copy(table, labels, sems.at[0])
    fetch.start()
    fetch_columns = pltpu.make_async_copy(
        right.at[:, pl.ds(0, count * TILE_EDGE)], columns, sems.at[1]
    )
    fetch_columns.start()
    fetch.wait()
    me = lax.axis_index("dev")
    row = row_for(labels, me, ncd, me ^ step)
    fetch_rows = pltpu.make_async_copy(
        left.at[pl.ds(row * TILE_EDGE, TILE_EDGE), :], rows, sems.at[2]
    )
    fetch_rows.start()
    fetch_child = pltpu.make_async_copy(child.at[pl.ds(row * MT, count)], out, sems.at[3])
    fetch_child.start()
    fetch_columns.wait()
    fetch_rows.wait()
    product = jnp.dot(
        rows[...], columns[...], precision=lax.Precision.HIGHEST, preferred_element_type=jnp.float32
    )
    fetch_child.wait()
    for g in range(count):
        out[g] = out[g] - product[:, g * TILE_EDGE : (g + 1) * TILE_EDGE]


def first_tiles(labels, l_slab, u_slab, child_tiles, ncd, step, count):
    shape = (count, TILE_EDGE, TILE_EDGE)
    panel = l_slab.shape[1]
    arrays = (labels, l_slab, u_slab, child_tiles)
    return pl.pallas_call(
        functools.partial(first_kernel, ncd, step),
        in_specs=[pl.BlockSpec(memory_space=pl.ANY)] * 4,
        out_specs=pl.BlockSpec(memory_space=pltpu.VMEM),
        out_shape=jax.ShapeDtypeStruct(shape, jnp.float32),
        scratch_shapes=[
            pltpu.SMEM(labels.shape, labels.dtype),
            pltpu.VMEM((TILE_EDGE, panel), jnp.float32),
            pltpu.VMEM((panel, count * TILE_EDGE), jnp.float32),
            pltpu.SemaphoreType.DMA((4,)),
        ],
        compiler_params=pltpu.CompilerParams(vmem_limit_bytes=8 * MIB),
    )(*(in_hbm(x) for x in arrays))


def start_front_kernel(ncd, labels, me, own, tiles, out):
    out[...] = own[...]

    @pl.when(pl.program_id(0) == parent_row(labels, me[0], ncd, me[0]))
    def _():
        def add(j, carry):
            at = labels[me[0] // ncd, j]
            out[at] = out[at] + tiles[j]
            return carry

        lax.fori_loop(0, MT, add, 0)


def start_front(labels, me, own, tiles, ncd):
    block = (PT, TILE_EDGE, TILE_EDGE)
    grid_spec = pltpu.PrefetchScalarGridSpec(
        num_scalar_prefetch=2,
        grid=(own.shape[0] // PT,),
        in_specs=[
            pl.BlockSpec(block, lambda q, lab, who: (q, 0, 0)),
            pl.BlockSpec(tiles.shape, lambda q, lab, who: (0, 0, 0)),
        ],
        out_specs=pl.BlockSpec(block, lambda q, lab, who: (q, 0, 0)),
    )
    return pl.pallas_call(
        functools.partial(start_front_kernel, ncd),
        grid_spec=grid_spec,
        out_shape=jax.ShapeDtypeStruct(own.shape, own.dtype),
        compiler_params=pltpu.CompilerParams(vmem_limit_bytes=VMEM_LIMIT),
        name="start_front",
    )(labels, me, in_hbm(own), tiles)


def each(count, action):
    def one(i, carry):
        action(i)
        return carry

    lax.fori_loop(0, count, one, 0)


def slots_of(ncd, step, first, labels, me, front):
    source = me ^ step
    base = parent_row(labels, me, ncd, source) * PT
    child = source // ncd
    return lambda i: front.at[base + labels[child, first + i]]


def extend_kernel(ncd, step, first, labels, me, tiles, front_in, after, front, sums, sems):
    slot = slots_of(ncd, step, first, labels, me[0], front)
    count = tiles.shape[0]
    each(count, lambda i: pltpu.make_async_copy(slot(i), sums.at[i], sems.at[0]).start())
    pltpu.make_async_copy(sums, sums, sems.at[0]).wait()

    def add(i):
        sums[i] = sums[i] + tiles[i]
        pltpu.make_async_copy(sums.at[i], slot(i), sems.at[1]).start()

    each(count, add)
    pltpu.make_async_copy(sums, sums, sems.at[1]).wait()


def extend(labels, me, tiles, front, after, ncd, step, first):
    grid_spec = pltpu.PrefetchScalarGridSpec(
        num_scalar_prefetch=2,
        grid=(1,),
        in_specs=[
            pl.BlockSpec(tiles.shape, lambda i, lab, who: (0, 0, 0)),
            pl.BlockSpec(memory_space=pl.ANY),
            pl.BlockSpec(memory_space=pl.ANY),
        ],
        out_specs=pl.BlockSpec(memory_space=pl.ANY),
        scratch_shapes=[
            pltpu.VMEM(tiles.shape, jnp.float32),
            pltpu.SemaphoreType.DMA((2,)),
        ],
    )
    return pl.pallas_call(
        functools.partial(extend_kernel, ncd, step, first),
        grid_spec=grid_spec,
        out_shape=jax.ShapeDtypeStruct(front.shape, front.dtype),
        input_output_aliases={3: 0},
        compiler_params=pltpu.CompilerParams(vmem_limit_bytes=8 * MIB),
    )(labels, me, tiles, front, after)


def take_kernel(ncd, step, first, labels, me, front, out, sem):
    slot = slots_of(ncd, step, first, labels, me[0], front)
    each(out.shape[0], lambda i: pltpu.make_async_copy(slot(i), out.at[i], sem.at[0]).start())
    pltpu.make_async_copy(out, out, sem.at[0]).wait()


def put_kernel(ncd, step, first, labels, me, tiles, old, front_in, front, sums, sem):
    slot = slots_of(ncd, step, first, labels, me[0], front)

    def add(i):
        sums[i] = old[i] + tiles[i]
        pltpu.make_async_copy(sums.at[i], slot(i), sem.at[0]).start()

    each(tiles.shape[0], add)
    pltpu.make_async_copy(sums, sums, sem.at[0]).wait()


def take(labels, me, front, ncd, step, first, count):
    shape = (count, TILE_EDGE, TILE_EDGE)
    grid_spec = pltpu.PrefetchScalarGridSpec(
        num_scalar_prefetch=2,
        grid=(1,),
        in_specs=[pl.BlockSpec(memory_space=pl.ANY)],
        out_specs=pl.BlockSpec(shape, lambda i, lab, who: (0, 0, 0)),
        scratch_shapes=[pltpu.SemaphoreType.DMA((1,))],
    )
    return pl.pallas_call(
        functools.partial(take_kernel, ncd, step, first),
        grid_spec=grid_spec,
        out_shape=jax.ShapeDtypeStruct(shape, jnp.float32),
        compiler_params=pltpu.CompilerParams(vmem_limit_bytes=50 * MIB),
    )(labels, me, in_hbm(front))


def put(labels, me, tiles, old, front, ncd, step, first):
    block = pl.BlockSpec(memory_space=pltpu.VMEM)
    grid_spec = pltpu.PrefetchScalarGridSpec(
        num_scalar_prefetch=2,
        in_specs=[block, block, pl.BlockSpec(memory_space=pl.ANY)],
        out_specs=pl.BlockSpec(memory_space=pl.ANY),
        scratch_shapes=[
            pltpu.VMEM(tiles.shape, jnp.float32),
            pltpu.SemaphoreType.DMA((1,)),
        ],
    )
    return pl.pallas_call(
        functools.partial(put_kernel, ncd, step, first),
        grid_spec=grid_spec,
        out_shape=jax.ShapeDtypeStruct(front.shape, front.dtype),
        input_output_aliases={4: 0},
        compiler_params=pltpu.CompilerParams(vmem_limit_bytes=3 * MIB),
    )(labels, me, tiles, old, front)


SENDS = (
    (6, 0, 2, 2),
    (6, 2, 6, 2),
    (6, 8, 24, 8),
    (4, 0, 32, 8),
    (5, 0, 32, 8),
    (7, 0, 28, 4),
    (7, 28, 4, 4),
    (1, 0, 32, 8),
    (2, 0, 32, 8),
    (3, 0, 32, 8),
)
ADDS = ((1, 0), (6, 0), (6, 2), (6, 8), (2, 0), (3, 0), (4, 0), (5, 0), (7, 0))
LAST = (7, 28)


def body_rows(child_tiles, l_slab, u_slab, parent_own_entries, parent_label):
    ndev = lax.axis_size("dev")
    ncd = ndev // 2
    me = lax.axis_index("dev").astype(jnp.int32).reshape(1)
    arrived = {}
    for step, first, count, group in SENDS:
        if not arrived:
            tiles = first_tiles(parent_label, l_slab, u_slab, child_tiles, ncd, step, count)
        else:
            tiles = stripe(
                parent_label,
                me,
                l_slab,
                u_slab,
                child_tiles,
                ncd,
                step,
                first,
                count,
                group,
            )
        pairs = [(d, d ^ step) for d in range(ndev)]
        arrived[step, first] = lax.ppermute(tiles, "dev", pairs)
    kept = stripe(parent_label, me, l_slab, u_slab, child_tiles, ncd, 0, 0, MT, 8)
    front = start_front(parent_label, me, parent_own_entries, kept, ncd)
    for step, first in ADDS[:-1]:
        tiles = arrived[step, first]
        front = extend(parent_label, me, tiles, front, parent_label, ncd, step, first)
    tiles = arrived[LAST]
    old = take(parent_label, me, front, ncd, *LAST, tiles.shape[0])
    step, first = ADDS[-1]
    front = extend(parent_label, me, arrived[step, first], front, old, ncd, step, first)
    return put(parent_label, me, tiles, old, front, ncd, *LAST)


def tile_targets(labels, count, ndev, me_index):
    cgc = ndev // 8
    pcols = ndev // 8
    ncd = ndev // 2
    cols_loc = MT // cgc
    inner = me_index % ncd
    local = jnp.arange(count, dtype=jnp.int32)
    tile_row = inner // cgc + CGR * (local // cols_loc)
    tile_col = inner % cgc + cgc * (local % cols_loc)
    columns = jnp.arange(MT, dtype=jnp.int32)
    label_row = jnp.sum(
        jnp.where(tile_row[:, None] == columns[None, :], labels[None, :], 0), axis=1
    )
    label_col = jnp.sum(
        jnp.where(tile_col[:, None] == columns[None, :], labels[None, :], 0), axis=1
    )
    dest_dev = label_row % PR * pcols + label_col % pcols
    dest_slot = label_row // PR * (PT // pcols) + label_col // pcols
    return (dest_dev, dest_slot)


def update_tiles(child_part, left_rows, u_slab, cols_loc):
    product = jnp.dot(
        left_rows, u_slab, precision=lax.Precision.HIGHEST, preferred_element_type=jnp.float32
    )
    row_tiles = left_rows.shape[0] // TILE_EDGE
    product = (
        product.reshape(row_tiles, TILE_EDGE, cols_loc, TILE_EDGE)
        .transpose(0, 2, 1, 3)
        .reshape(row_tiles * cols_loc, TILE_EDGE, TILE_EDGE)
    )
    return child_part - product


def pack_tiles(updated, dest_dev, dest_slot, ndev, bound):
    count = updated.shape[0]
    order = jnp.arange(count, dtype=jnp.int32)
    earlier = order[None, :] < order[:, None]
    same_dest = dest_dev[:, None] == dest_dev[None, :]
    arrival = jnp.sum(jnp.where(same_dest & earlier, 1, 0), axis=1).astype(jnp.int32)
    position = dest_dev * bound + arrival
    places = jnp.arange(ndev * bound, dtype=jnp.int32)
    hits = places[:, None] == position[None, :]
    select = hits.astype(jnp.float32)
    packed = jnp.dot(
        select,
        updated.reshape(count, -1),
        precision=lax.Precision.HIGHEST,
        preferred_element_type=jnp.float32,
    )
    filled = jnp.sum(jnp.where(hits, 1, 0), axis=1)
    sent_slot = jnp.where(filled > 0, jnp.sum(jnp.where(hits, dest_slot[None, :], 0), axis=1), -1)
    return (packed.reshape(ndev, bound, -1), sent_slot.reshape(ndev, bound))


def assemble_front(incoming_tiles, incoming_slot, slot_count):
    flat = incoming_tiles.reshape(-1, incoming_tiles.shape[-1])
    select = (
        jnp.arange(slot_count, dtype=jnp.int32)[:, None] == incoming_slot.reshape(-1)[None, :]
    ).astype(jnp.float32)
    return jnp.dot(
        select, flat, precision=lax.Precision.HIGHEST, preferred_element_type=jnp.float32
    )


def body_grid(child_tiles, l_slab, u_slab, parent_own_entries, parent_label):
    ndev = lax.axis_size("dev")
    me_index = lax.axis_index("dev")
    cgc = ndev // 8
    pcols = ndev // 8
    bound = max(1, MT // (cgc * pcols))
    cols_loc = MT // cgc
    tiles_dev = child_tiles.shape[0]
    slot_count = parent_own_entries.shape[0]
    child_id = me_index // (ndev // 2)
    labels = lax.dynamic_index_in_dim(parent_label, child_id, 0, keepdims=False)
    updated = update_tiles(child_tiles, l_slab, u_slab, cols_loc)
    dest_dev, dest_slot = tile_targets(labels, tiles_dev, ndev, me_index)
    packed, sent_slot = pack_tiles(updated, dest_dev, dest_slot, ndev, bound)
    incoming_tiles, incoming_slot = (
        lax.all_to_all(packed, "dev", split_axis=0, concat_axis=0, tiled=True),
        lax.all_to_all(sent_slot, "dev", split_axis=0, concat_axis=0, tiled=True),
    )
    summed_entries = assemble_front(incoming_tiles, incoming_slot, slot_count)
    return parent_own_entries + summed_entries.reshape(slot_count, TILE_EDGE, TILE_EDGE)


def solution(mesh):
    in_specs = (
        P(("sub", "dev"), None, None),
        P(("sub", "dev"), None),
        P(None, ("sub", "dev")),
        P(("sub", "dev"), None, None),
        P("sub", None),
    )
    out_specs = P(("sub", "dev"), None, None)
    rows_only = mesh.shape["dev"] == PR
    body = body_rows if rows_only else body_grid
    return jax.shard_map(body, mesh=mesh, in_specs=in_specs, out_specs=out_specs, check_vma=False)
```
